32 devices in a mesh: dp: 8 (over z, x), mp: 4 (over y, core).
Axes of the slice: x: 2, y: 2, z: 4, core: 2. Of those that a mesh axis runs over, the one named last changes fastest.
Arguments:
- acts: bfloat16 [1, 16384, 4096], P(None, 'dp'), may hold values from -64 to 64
- out_grads: bfloat16 [1, 16384, 4096], P(None, 'dp', 'mp'), may hold values from -80 to 80
- clip_bound: float32 [1], replicated, may hold values from 163840 to 491520
- noise: float32 [1, 4096, 4096], P(None, 'dp', 'mp'), may hold values from -6 to 6
Outputs:
- update: float32 [1, 4096, 4096], P(None, 'dp', 'mp')
The draws below stay inside these ranges and needn't reach their ends.
All inputs are finite; a program needn't handle non-finite values.
Results may differ from the reference program's by a relative error of at most 0.0017.
Values may be sent and summed in bfloat16 or wider, within the bound.
A program may use at most 128 MiB of HBM per device.

```python
import math
import jax
import jax.numpy as jnp
from jax import lax

D = 4096
GROUPS = 1
SEQ = 512
BATCH = 32
TOKENS = 16384


def token_signs(key):
    sign_key = jax.random.fold_in(key, 37)
    flips = jax.random.bernoulli(sign_key, 0.5, (GROUPS, BATCH, SEQ, 1))
    return jnp.where(flips, 1.0, -1.0).astype(jnp.float32)


def draw_acts(key, part):
    base_key = jax.random.fold_in(key, 11)
    key_rows, key_cols, key_base = jax.random.split(base_key, 3)
    key_direction = jax.random.fold_in(base_key, 5)
    row_scale = jnp.exp(jax.random.uniform(key_rows, (GROUPS, TOKENS, 1), jnp.float32, math.log(0.3), math.log(3.0)))
    col_scale = jnp.exp(jax.random.uniform(key_cols, (GROUPS, 1, D), jnp.float32, math.log(0.3), math.log(3.0)))
    direction = jnp.clip(jax.random.normal(key_direction, (GROUPS, BATCH, 1, D), jnp.float32), -2.5, 2.5)
    shared = (0.35 * token_signs(key) * direction).reshape(GROUPS, TOKENS, D)
    base_draw = jnp.clip(jax.random.normal(key_base, (GROUPS, TOKENS, D), jnp.float32), -6.0, 6.0)
    return ((base_draw + shared) * row_scale * col_scale).astype(jnp.bfloat16)


def draw_out_grads(key, part):
    base_key = jax.random.fold_in(key, 23)
    key_examples, key_rows, key_cols, key_base = jax.random.split(base_key, 4)
    key_direction = jax.random.fold_in(base_key, 7)
    example_scale = jnp.exp(jax.random.uniform(key_examples, (GROUPS, BATCH, 1, 1), jnp.float32, math.log(0.3), math.log(3.0)))
    row_scale = jnp.exp(jax.random.uniform(key_rows, (GROUPS, BATCH, SEQ, 1), jnp.float32, math.log(0.5), math.log(2.0)))
    col_scale = jnp.exp(jax.random.uniform(key_cols, (GROUPS, 1, 1, D), jnp.float32, math.log(0.5), math.log(2.0)))
    direction = jnp.clip(jax.random.normal(key_direction, (GROUPS, BATCH, 1, D), jnp.float32), -2.5, 2.5)
    shared = 0.25 * token_signs(key) * direction
    base_draw = jnp.clip(jax.random.normal(key_base, (GROUPS, BATCH, SEQ, D), jnp.float32), -6.0, 6.0)
    values = (base_draw + shared) * example_scale * row_scale * col_scale
    return values.reshape(GROUPS, TOKENS, D).astype(jnp.bfloat16)


def block_scale(rng, dims, cuts, smallest, largest):
    factor_of = 1.0
    for position, blocks in cuts:
        heights = jax.random.uniform(jax.random.fold_in(jax.random.fold_in(rng, 6), position), (blocks,), jnp.float32, smallest / len(cuts), largest / len(cuts))
        factor_of = factor_of * jnp.repeat(jnp.exp(heights), dims[position] // blocks).reshape((-1,) + (1,) * (len(dims) - 1 - position))
    return factor_of


def bell_draw(rng, shape, spread, reach, pieces=(), held_as=jnp.bfloat16):
    values = spread * jax.random.normal(rng, shape, jnp.float32)
    if pieces:
        values = values * block_scale(rng, shape, pieces, -0.22, 0.18)
    return jnp.clip(values, -reach, reach).astype(held_as)


def setup_inputs(seed: int = 0) -> dict:
    key_of = jax.random.split(jax.random.key(seed), 5)
    acts = draw_acts(jax.random.fold_in(key_of[4], 71), 0)
    out_grads = draw_out_grads(jax.random.fold_in(key_of[4], 71), 0)
    clip_bound = jnp.clip(jnp.exp(jax.random.uniform(key_of[2], (GROUPS,), jnp.float32, math.log(163840.0), math.log(491520.0))), 163840.0, 491520.0)
    noise = bell_draw(key_of[3], (GROUPS, D, D), 0.5, 6.0, ((1, 8), (2, 4)), jnp.float32)
    return {"acts": acts, "out_grads": out_grads, "clip_bound": clip_bound, "noise": noise}


def reference(acts, out_grads, clip_bound, noise):
    results = []
    for group_index in range(GROUPS):
        act_seq = acts[group_index].reshape(BATCH, SEQ, D)
        grad_seq = out_grads[group_index].reshape(BATCH, SEQ, D)

        def one_example(pair):
            act_one, grad_one = pair
            gram_act = jnp.dot(act_one, act_one.T, preferred_element_type=jnp.float32)
            gram_grad = jnp.dot(grad_one, grad_one.T, preferred_element_type=jnp.float32)
            return jnp.sum(gram_act * gram_grad)
        norm_sq = lax.map(one_example, (act_seq, grad_seq))
        bound = clip_bound[group_index]
        clip = jnp.minimum(1.0, bound / jnp.sqrt(norm_sq + 1e-06))
        factor = clip / bound
        scaled = (grad_seq.astype(jnp.float32) * factor[:, None, None]).astype(jnp.bfloat16)
        scaled = scaled.reshape(TOKENS, D)
        summed = jnp.dot(acts[group_index].T, scaled, preferred_element_type=jnp.float32)
        results.append(summed * (D / math.sqrt(BATCH)) + noise[group_index])
    return jnp.stack(results)
```

```python
import functools
import math

import jax
import jax.numpy as jnp
from jax import lax
from jax.experimental import pallas as pl
from jax.experimental.pallas import tpu as pltpu
from jax.sharding import PartitionSpec as P

SEQ = 512
NT = (((1,), (1,)), ((), ()))
MESH = pl.DeviceIdType.MESH
LIFT = 2.0**50


def coded(value):
    lifted = value * LIFT
    return (lifted * jnp.abs(lifted)).astype(jnp.bfloat16)


def decoded(code):
    code = code.astype(jnp.float32)
    return code * lax.rsqrt(jnp.maximum(jnp.abs(code), 1e-37)) * (1.0 / LIFT)


def kernel(
    groups, lanes, acts_hbm, grads_hbm, bound_ref, out_hbm,
    acts, grads, grads_t, xs, xr, zs, zr, norm_mine, norm_peer, total, out,
    load_sem, out_sem, norm_send, norm_recv, x_send, x_recv, z_send, z_recv,
):
    planes = groups // 2
    steps = 2 * planes
    feats = acts.shape[1] // groups
    half_cols = grads.shape[1] // 2
    examples = acts.shape[0] // SEQ
    me = lax.axis_index("dp")
    lane = lax.axis_index("mp")
    line, pair = me // 2, me % 2
    has_below = (line > 0).astype(jnp.int32)
    has_above = (line < planes - 1).astype(jnp.int32)
    x_peer = {"dp": line * 2 + 1 - pair}
    above = {"dp": jnp.minimum(line + 1, planes - 1) * 2 + pair}
    below = {"dp": jnp.maximum(line - 1, 0) * 2 + pair}

    def rows_of(e):
        return pl.ds(pl.multiple_of(e * SEQ, SEQ), SEQ)

    def load(e, which):
        source, target = (grads_hbm, grads) if which else (acts_hbm, acts)
        return pltpu.make_async_copy(
            source.at[rows_of(e)], target.at[rows_of(e)], load_sem.at[which, e]
        )

    for e in range(examples):
        load(e, 1).start()
        load(e, 0).start()

    barrier = pltpu.get_barrier_semaphore()
    pl.semaphore_signal(barrier, inc=1, device_id=x_peer, device_id_type=MESH)
    for j in range(1, lanes):
        pl.semaphore_signal(
            barrier, inc=1, device_id={"mp": lax.rem(lane + j, lanes)}, device_id_type=MESH
        )

    @pl.when(line > 0)
    def _():
        pl.semaphore_signal(barrier, inc=1, device_id=below, device_id_type=MESH)

    @pl.when(line < planes - 1)
    def _():
        pl.semaphore_signal(barrier, inc=1, device_id=above, device_id_type=MESH)

    cut = SEQ // 2

    def gram(ref, e):
        base = pl.multiple_of(e * SEQ, SEQ)
        low, high = ref[pl.ds(base, cut), :], ref[pl.ds(base + cut, cut), :]
        dot = functools.partial(
            lax.dot_general, dimension_numbers=NT, preferred_element_type=jnp.float32
        )
        return dot(low, low), dot(low, high), dot(high, high)

    def norm_step(e, carry):
        load(e, 1).wait()
        gg = gram(grads, e)
        load(e, 0).wait()
        ga = gram(acts, e)
        prod = ga[0] * gg[0] + 2.0 * (ga[1] * gg[1]) + ga[2] * gg[2]
        norm_mine[e] = jnp.broadcast_to(jnp.sum(prod, keepdims=True), norm_mine.shape[1:])
        return carry

    lax.fori_loop(0, examples, norm_step, 0)
    pl.semaphore_wait(barrier, lanes + has_below + has_above)

    def norm_copy(j):
        return pltpu.make_async_remote_copy(
            src_ref=norm_mine, dst_ref=norm_peer.at[j - 1],
            send_sem=norm_send.at[j - 1], recv_sem=norm_recv.at[j - 1],
            device_id={"mp": lax.rem(lane + j, lanes)}, device_id_type=MESH,
        )

    for j in range(1, lanes):
        norm_copy(j).start()
    for j in range(1, lanes):
        norm_copy(j).wait()

    bound = bound_ref[0]

    def scale_step(e, carry):
        norm_sq = norm_mine[e]
        for j in range(1, lanes):
            norm_sq = norm_sq + norm_peer[j - 1, e]
        factor = (jnp.minimum(1.0, bound / jnp.sqrt(norm_sq + 1e-06)) / bound)[:1, :1]
        scaled = (grads[rows_of(e), :].astype(jnp.float32) * factor).astype(jnp.bfloat16)
        grads_t[:, rows_of(e)] = scaled.T
        return carry

    lax.fori_loop(0, examples, scale_step, 0)

    def target_of(k):
        ups = planes - 1 - line
        up_first = jnp.where(k < ups, planes - 1 - k, k - ups)
        down_first = jnp.where(k < line, k, planes - 1 - (k - line))
        ordered = jnp.where(line < planes // 2, up_first, down_first)
        return jnp.where(k == planes - 1, line, ordered)

    def term(block, half):
        cols = pl.ds(pl.multiple_of(block * feats, feats), feats)
        rows = pl.ds(pl.multiple_of(half * half_cols, half_cols), half_cols)
        return jnp.dot(grads_t[rows, :], acts[:, cols], preferred_element_type=jnp.float32)

    def x_copy(s):
        return pltpu.make_async_remote_copy(
            src_ref=xs.at[s], dst_ref=xr.at[s], send_sem=x_send.at[s], recv_sem=x_recv.at[s],
            device_id=x_peer, device_id_type=MESH,
        )

    def z_copy(s, slot, device):
        return pltpu.make_async_remote_copy(
            src_ref=zs.at[s], dst_ref=zr.at[slot], send_sem=z_send.at[s],
            recv_sem=z_recv.at[slot], device_id=device, device_id_type=MESH,
        )

    def send_step(s, carry):
        xs[s] = coded(term(target_of(s // 2) * 2 + 1 - pair, s % 2))
        x_copy(s).start()
        return carry

    lax.fori_loop(0, steps, send_step, 0)

    def add_arrival(slot):
        z_copy(0, slot, above).wait_recv()
        total[...] += decoded(zr[slot])

    def sum_step(s, carry):
        target, half = target_of(s // 2), s % 2
        slot = target * 2 + half
        own = term(target * 2 + pair, half)
        x_copy(s).wait_recv()
        total[...] = own + decoded(xr[s])

        @pl.when((target >= line) & (line > 0))
        def _():
            add_arrival(slot)

        @pl.when((target < line) & (line < planes - 1))
        def _():
            add_arrival(slot)

        @pl.when((target == line) & (line < planes - 1))
        def _():
            add_arrival(steps + half)

        @pl.when(target > line)
        def _():
            zs[s] = coded(total[...])
            z_copy(s, slot, above).start()

        @pl.when(target < line)
        def _():
            zs[s] = coded(total[...])
            z_copy(s, jnp.where(target == line - 1, steps + half, slot), below).start()

        @pl.when(target == line)
        def _():
            cols = pl.ds(pl.multiple_of(half * half_cols, half_cols), half_cols)
            out[:, cols] = total[...].T
            pltpu.make_async_copy(out.at[:, cols], out_hbm.at[:, cols], out_sem.at[half]).start()

        return carry

    lax.fori_loop(0, steps, sum_step, 0)

    def drain_step(s, carry):
        x_copy(s).wait_send()

        @pl.when(s < steps - 2)
        def _():
            z_copy(s, 0, above).wait_send()

        return carry

    lax.fori_loop(0, steps, drain_step, 0)
    for half in range(2):
        cols = pl.ds(half * half_cols, half_cols)
        pltpu.make_async_copy(out.at[:, cols], out_hbm.at[:, cols], out_sem.at[half]).wait()


def clipped_sum(act_block, grad_block, bound):
    groups, lanes = lax.axis_size("dp"), lax.axis_size("mp")
    tokens, width = act_block.shape
    cols = grad_block.shape[1]
    feats = width // groups
    steps = groups
    examples = tokens // SEQ
    half = (cols // 2, feats)
    dma = pltpu.SemaphoreType.DMA
    any_space = pl.BlockSpec(memory_space=pl.ANY)
    return pl.pallas_call(
        functools.partial(kernel, groups, lanes),
        out_shape=jax.ShapeDtypeStruct((feats, cols), jnp.float32),
        in_specs=[any_space, any_space, pl.BlockSpec(memory_space=pltpu.SMEM)],
        out_specs=any_space,
        scratch_shapes=[
            pltpu.VMEM((tokens, width), jnp.bfloat16),
            pltpu.VMEM((tokens, cols), jnp.bfloat16),
            pltpu.VMEM((cols, tokens), jnp.bfloat16),
            pltpu.VMEM((steps,) + half, jnp.bfloat16),
            pltpu.VMEM((steps,) + half, jnp.bfloat16),
            pltpu.VMEM((steps,) + half, jnp.bfloat16),
            pltpu.VMEM((steps + 2,) + half, jnp.bfloat16),
            pltpu.VMEM((examples, 8, 128), jnp.float32),
            pltpu.VMEM((max(lanes - 1, 1), examples, 8, 128), jnp.float32),
            pltpu.VMEM(half, jnp.float32),
            pltpu.VMEM((feats, cols), jnp.float32),
            dma((2, examples)),
            dma((2,)),
            dma((max(lanes - 1, 1),)),
            dma((max(lanes - 1, 1),)),
            dma((steps,)),
            dma((steps,)),
            dma((steps,)),
            dma((steps + 2,)),
        ],
        compiler_params=pltpu.CompilerParams(
            collective_id=0, has_side_effects=True, vmem_limit_bytes=60 * 2**20
        ),
        name="clipped_sum",
    )(act_block, grad_block, bound)


def on_device(acts, out_grads, clip_bound, noise):
    model_width = acts.shape[2]
    batch_total = acts.shape[1] // SEQ * lax.axis_size("dp")
    out_factor = model_width / math.sqrt(batch_total)
    updates = [
        clipped_sum(acts[g], out_grads[g], clip_bound[g : g + 1]) * out_factor + noise[g]
        for g in range(acts.shape[0])
    ]
    return jnp.stack(updates)


def solution(mesh):
    placed = (P(None, "dp", None), P(None, "dp", "mp"), P(), P(None, "dp", "mp"))
    return jax.shard_map(
        on_device, mesh=mesh, in_specs=placed, out_specs=P(None, "dp", "mp"), check_vma=False
    )
```
